32 devices in a mesh: rep: 4 (over x, y), pp: 8 (over z, core).
Axes of the slice: x: 2, y: 2, z: 4, core: 2. Of those that a mesh axis runs over, the one named last changes fastest.
Arguments:
- x: bfloat16 [64, 512, 512], P('rep'), parts along dimension 0
- dy: bfloat16 [64, 512, 512], P('rep'), parts along dimension 0
- w_gate: bfloat16 [8, 512, 1280], P('pp')
- w_up: bfloat16 [8, 512, 1280], P('pp')
- w_down: bfloat16 [8, 1280, 512], P('pp')
Outputs:
- output 1: bfloat16 [32, 512, 1280], P(('rep', 'pp')), parts along dimension 0
- output 2: bfloat16 [32, 512, 1280], P(('rep', 'pp')), parts along dimension 0
- output 3: bfloat16 [32, 1280, 512], P(('rep', 'pp')), parts along dimension 0
There are 4 independent parts. The reference program is written for one: setup_inputs(seed, part) draws one part's arguments, and reference() takes and returns one part's arrays. A program takes and returns all parts, laid end to end along the dimension named above; an argument that names none is the same for every part.
All inputs are finite; a program needn't handle non-finite values.
Results may differ from the reference program's by a relative error of at most 0.0266.
Values are sent between devices in bfloat16 or wider.
A program may use at most 2 GiB of HBM per device.

```python
import jax
import jax.numpy as jnp
from jax import lax

MICRO = 16
TOKENS = 512
D = 512
FF = 1280
LAYERS = 8
NAMES = ("w_gate", "w_up", "w_down")
SHAPES = {"w_gate": (LAYERS, D, FF), "w_up": (LAYERS, D, FF), "w_down": (LAYERS, FF, D)}


def bump(key, n, height):
    away = (jnp.arange(n, dtype=jnp.int32) - jax.random.randint(key, (), 0, n, jnp.int32)) % n
    return jnp.where(away < n // 8, height, 1.0)


def together(key, own, strength):
    shared = jax.random.normal(key, own.shape[1:], jnp.float32)
    return (own + strength * shared) * lax.rsqrt(1 + strength * strength)


def setup_inputs(seed: int = 0, part: int = 0) -> dict:
    kx, kdy, ka, kb, kz, kf, kh, kl, *kw = jax.random.split(jax.random.key(seed), 8 + len(NAMES))
    kx, kdy, ka, kb = (jax.random.fold_in(k, part) for k in (kx, kdy, ka, kb))
    shape = (MICRO, TOKENS, D)
    much_x, much_dy = jax.random.uniform(kz, (2,), jnp.float32, 0.0, 1.0)
    layers = 2.0 ** jax.random.uniform(kl, (LAYERS, 1, 1), jnp.float32, -1.0, 1.0)
    x = together(ka, jax.random.normal(kx, shape, jnp.float32), much_x) * bump(kf, D, 4.0)
    dy = together(kb, jax.random.normal(kdy, shape, jnp.float32), much_dy)
    drawn = {"x": x.astype(jnp.bfloat16), "dy": (dy * (MICRO * TOKENS) ** -0.5).astype(jnp.bfloat16)}
    for key, name in zip(kw, NAMES, strict=True):
        w = jax.random.normal(key, SHAPES[name], jnp.float32) * SHAPES[name][1] ** -0.5
        drawn[name] = (w * {"w_gate": 1.0, "w_up": bump(kh, FF, 4.0), "w_down": layers}[name]).astype(jnp.bfloat16)
    return drawn


def matmul(a, w):
    return jnp.dot(a, w, preferred_element_type=jnp.float32).astype(jnp.bfloat16)


def normed(h):
    wide = h.astype(jnp.float32)
    scale = lax.rsqrt(jnp.mean(wide**2, -1, keepdims=True) + 1e-6)
    return (wide * scale).astype(jnp.bfloat16)


def layer(h, w):
    a = normed(h)
    gate = jnp.dot(a, w["w_gate"], preferred_element_type=jnp.float32)
    up = jnp.dot(a, w["w_up"], preferred_element_type=jnp.float32)
    return h + matmul((jax.nn.silu(gate) * up).astype(jnp.bfloat16), w["w_down"])


def stack(weights, h):
    return lax.scan(lambda h, w: (layer(h, w), None), h, weights)[0]


def reference(x, dy, w_gate, w_up, w_down):
    weights = dict(zip(NAMES, (w_gate, w_up, w_down), strict=True))

    def take(so_far, one):
        h, by_y = one
        _, back = jax.vjp(lambda w: stack(w, h), weights)
        return jax.tree.map(lambda total, term: total + term.astype(jnp.float32), so_far, back(by_y)[0]), None

    none_yet = {name: jnp.zeros(w.shape, jnp.float32) for name, w in weights.items()}
    by_weights, _ = lax.scan(take, none_yet, (x, dy))
    return tuple(by_weights[name].astype(jnp.bfloat16) for name in NAMES)
```

```python
import functools

import jax
import jax.numpy as jnp
from jax import lax
from jax.experimental import pallas as pl
from jax.experimental.pallas import tpu as pltpu
from jax.sharding import PartitionSpec as P

f32, bf16 = jnp.float32, jnp.bfloat16
MESH = pl.DeviceIdType.MESH
PARTS = 2
RING_F, RING_B = 4, 2
SENDS = 4
LATE = 3
STAGES = 8


def ahead_of(me):
    return (3 * (STAGES - 1 - me)) // 2


def late_of(me):
    return jnp.clip(me - 4, 0, LATE)


def dot(a, b):
    return jnp.dot(a, b, preferred_element_type=f32)


def dot_t(a, b):
    return lax.dot_general(a, b, (((1,), (1,)), ((), ())), preferred_element_type=f32)


def scale_of(wide):
    return lax.rsqrt(jnp.mean(wide * wide, -1, keepdims=True) + 1e-6)


def kernel(
    x, dy, w_gate, w_up, w_down, by_gate, by_up, by_down, spill,
    wg, wu, wd, hs, ds, ring, ps, dgs, dus, a_t, dy_t, out_f, out_b, sum_g, sum_u, sum_d,
    w_sem, f_recv, b_recv, f_send, b_send, spill_sem, fetch_sem, end_sem,
):
    micro, tokens, d = hs.shape
    ff = wg.shape[1]
    wide_block = 256 if ff % 256 == 0 else 128
    rows_n = tokens // PARTS
    chunks = micro * PARTS
    me = lax.axis_index("pp")
    first, last = me == 0, me == STAGES - 1
    ahead, late = ahead_of(me), late_of(me)
    resident = 2 * ahead + 1 <= RING_F + RING_B

    def rows_of(c):
        return pl.ds(c * rows_n, rows_n)

    def weights_in():
        return [
            pltpu.make_async_copy(src.at[0], dst, w_sem.at[i])
            for i, (src, dst) in enumerate(((w_gate, wg), (w_up, wu), (w_down, wd)))
        ]

    def load_x(t, c):
        return pltpu.make_async_copy(x.at[t, rows_of(c)], hs.at[t, rows_of(c)], f_recv.at[t * PARTS + c])

    def load_dy(t, c):
        return pltpu.make_async_copy(dy.at[t, rows_of(c)], ds.at[t, rows_of(c)], b_recv.at[t * PARTS + c])

    def onward(t, c):
        i = t * PARTS + c
        return pltpu.make_async_remote_copy(
            src_ref=out_f.at[i % SENDS],
            dst_ref=hs.at[t, rows_of(c)],
            send_sem=f_send.at[i % SENDS],
            recv_sem=f_recv.at[i],
            device_id={"pp": me + 1},
            device_id_type=MESH,
        )

    def back_again(t, c):
        i = t * PARTS + c
        return pltpu.make_async_remote_copy(
            src_ref=out_b.at[i % SENDS],
            dst_ref=ds.at[t, rows_of(c)],
            send_sem=b_send.at[i % SENDS],
            recv_sem=b_recv.at[i],
            device_id={"pp": me - 1},
            device_id_type=MESH,
        )

    def put_away(i):
        return pltpu.make_async_copy(ring.at[i % RING_F], spill.at[i], spill_sem.at[i % RING_F])

    def fetch(i):
        return pltpu.make_async_copy(spill.at[i], ring.at[RING_F + i % RING_B], fetch_sem.at[i % RING_B])

    barrier = pltpu.get_barrier_semaphore()

    @pl.when(jnp.logical_not(last))
    def _():
        pl.semaphore_signal(barrier, inc=1, device_id={"pp": me + 1}, device_id_type=MESH)

    @pl.when(jnp.logical_not(first))
    def _():
        pl.semaphore_signal(barrier, inc=1, device_id={"pp": me - 1}, device_id_type=MESH)

    for copy in weights_in():
        copy.start()

    @pl.when(first)
    def _():
        @pl.loop(0, micro)
        def _(t):
            for c in range(PARTS):
                load_x(t, c).start()

    @pl.when(last)
    def _():
        @pl.loop(0, micro)
        def _(t):
            for c in range(PARTS):
                load_dy(t, c).start()

    for total in (sum_g, sum_u, sum_d):
        total[...] = jnp.zeros_like(total)
    for copy in weights_in():
        copy.wait()

    pl.semaphore_wait(barrier, jnp.where(first | last, 1, 2))

    def forward_math(t, c, slot, send):
        rows = rows_of(c)
        wide = hs[t, rows, :].astype(f32)
        a = (wide * scale_of(wide)).astype(bf16)
        products = []
        for n in range(ff // wide_block):
            cols = slice(n * wide_block, (n + 1) * wide_block)
            gate, up = dot(a, wg[:, cols]), dot(a, wu[:, cols])
            ring[slot, 0, :, cols] = gate
            ring[slot, 1, :, cols] = up
            if send:
                products.append((gate * jax.nn.sigmoid(gate) * up).astype(bf16))
        if send:
            y = dot(jnp.concatenate(products, -1), wd[...]).astype(bf16)
            out_f[(t * PARTS + c) % SENDS] = (wide + y.astype(f32)).astype(bf16)

    def forward(t, c):
        i = t * PARTS + c

        @pl.when(first)
        def _():
            load_x(t, c).wait()

        @pl.when(jnp.logical_not(first))
        def _():
            onward(t, c).wait_recv()

        @pl.when(jnp.logical_not(resident) & (i >= RING_F))
        def _():
            put_away(i - RING_F).wait()

        slot = jnp.where(resident, i % (RING_F + RING_B), i % RING_F)

        @pl.when(last)
        def _():
            forward_math(t, c, slot, False)

        @pl.when(jnp.logical_not(last))
        def _():
            @pl.when(i >= SENDS)
            def _():
                back = i - SENDS
                onward(back // PARTS, back % PARTS).wait_send()

            forward_math(t, c, slot, True)
            onward(t, c).start()

        @pl.when(jnp.logical_not(resident))
        def _():
            put_away(i).start()

    def backward_math(t, c, slot, send):
        rows = rows_of(c)
        at = t % (LATE + 1)
        by_y = ds[t, rows, :]
        for n in range(ff // wide_block):
            cols = slice(n * wide_block, (n + 1) * wide_block)
            by_product = dot_t(by_y, wd[cols, :]).astype(bf16).astype(f32)
            gate, up = ring[slot, 0, :, cols], ring[slot, 1, :, cols]
            sig = jax.nn.sigmoid(gate)
            silu = gate * sig
            ps[at, rows, cols] = (silu * up).astype(bf16)
            dus[at, rows, cols] = (by_product * silu).astype(bf16)
            dgs[at, rows, cols] = (by_product * up * (sig * (1.0 + gate * (1.0 - sig)))).astype(bf16)
        if send:
            by_a = (
                dot_t(dgs[at, rows, :], wg[...]).astype(bf16).astype(f32)
                + dot_t(dus[at, rows, :], wu[...]).astype(bf16).astype(f32)
            ).astype(bf16).astype(f32)
            wide = hs[t, rows, :].astype(f32)
            scale = scale_of(wide)
            pull = jnp.sum(by_a * wide, -1, keepdims=True) * (scale * scale * scale) * (-1.0 / d)
            by_h = (by_a * scale + wide * pull).astype(bf16)
            out_b[(t * PARTS + c) % SENDS] = (by_y.astype(f32) + by_h.astype(f32)).astype(bf16)

    def backward(t, c):
        i = t * PARTS + c

        @pl.when(last)
        def _():
            load_dy(t, c).wait()

        @pl.when(jnp.logical_not(last))
        def _():
            back_again(t, c).wait_recv()

        @pl.when(jnp.logical_not(resident))
        def _():
            fetch(i).wait()

            @pl.when(i + 1 < chunks)
            def _():
                fetch(i + 1).start()

        slot = jnp.where(resident, i % (RING_F + RING_B), RING_F + i % RING_B)

        @pl.when(first)
        def _():
            backward_math(t, c, slot, False)

        @pl.when(jnp.logical_not(first))
        def _():
            @pl.when(i >= SENDS)
            def _():
                back = i - SENDS
                back_again(back // PARTS, back % PARTS).wait_send()

            backward_math(t, c, slot, True)
            back_again(t, c).start()

    def by_weights(t):
        at = t % (LATE + 1)
        wide = hs[t].astype(f32)
        a_t[...] = (wide * scale_of(wide)).astype(bf16).T
        dy_t[...] = ds[t].T
        for total, left, right in ((sum_d, dy_t, ps), (sum_g, a_t, dgs), (sum_u, a_t, dus)):
            for n in range(ff // wide_block):
                cols = slice(n * wide_block, (n + 1) * wide_block)
                total[:, cols] += dot(left[...], right[at, :, cols]).astype(bf16).astype(f32)

    @pl.loop(0, micro + max(ahead_of(k) + max(0, min(k - 4, LATE)) for k in range(STAGES)))
    def _(t):
        u = t - ahead
        v = u - late

        @pl.when(jnp.logical_not(resident) & (t == micro))
        def _():
            for i in range(chunks - RING_F, chunks):
                put_away(i).wait()

        for c in range(PARTS):

            @pl.when(t < micro)
            def _(c=c):
                forward(t, c)

            @pl.when((u >= 0) & (u < micro))
            def _(c=c):
                backward(u, c)

        @pl.when(jnp.logical_not(resident) & (u == -1))
        def _():
            fetch(0).start()

        @pl.when((v >= 0) & (v < micro))
        def _():
            by_weights(v)

    copies = []
    for i, (total, to, out) in enumerate(((sum_g, dgs, by_gate), (sum_u, dus, by_up), (sum_d, ps, by_down))):
        to[0] = total[...].astype(bf16)
        copies.append(pltpu.make_async_copy(to.at[0], out.at[0], end_sem.at[i]))
        copies[-1].start()

    @pl.when(jnp.logical_not(last))
    def _():
        for i in range(chunks - SENDS, chunks):
            onward(i // PARTS, i % PARTS).wait_send()

    @pl.when(jnp.logical_not(first))
    def _():
        for i in range(chunks - SENDS, chunks):
            back_again(i // PARTS, i % PARTS).wait_send()

    for copy in copies:
        copy.wait()


def solution(mesh):
    def step(x, dy, w_gate, w_up, w_down):
        micro, tokens, d = x.shape
        ff = w_gate.shape[2]
        rows, chunks = tokens // PARTS, micro * PARTS
        flops = 9 * micro * 2 * tokens * d * ff
        anywhere = pl.BlockSpec(memory_space=pl.ANY)
        by_gate, by_up, by_down, _ = pl.pallas_call(
            kernel,
            out_shape=[jax.ShapeDtypeStruct((1, d, ff), bf16)] * 3
            + [jax.ShapeDtypeStruct((chunks, 2, rows, ff), f32)],
            in_specs=[anywhere] * 5,
            out_specs=[anywhere] * 4,
            scratch_shapes=[
                pltpu.VMEM((d, ff), bf16),
                pltpu.VMEM((d, ff), bf16),
                pltpu.VMEM((ff, d), bf16),
                pltpu.VMEM((micro, tokens, d), bf16),
                pltpu.VMEM((micro, tokens, d), bf16),
                pltpu.VMEM((RING_F + RING_B, 2, rows, ff), f32),
                *[pltpu.VMEM((LATE + 1, tokens, ff), bf16)] * 3,
                pltpu.VMEM((d, tokens), bf16),
                pltpu.VMEM((d, tokens), bf16),
                pltpu.VMEM((SENDS, rows, d), bf16),
                pltpu.VMEM((SENDS, rows, d), bf16),
                *[pltpu.VMEM((d, ff), f32)] * 3,
                pltpu.SemaphoreType.DMA((3,)),
                pltpu.SemaphoreType.DMA((chunks,)),
                pltpu.SemaphoreType.DMA((chunks,)),
                pltpu.SemaphoreType.DMA((SENDS,)),
                pltpu.SemaphoreType.DMA((SENDS,)),
                pltpu.SemaphoreType.DMA((RING_F,)),
                pltpu.SemaphoreType.DMA((RING_B,)),
                pltpu.SemaphoreType.DMA((3,)),
            ],
            compiler_params=pltpu.CompilerParams(
                collective_id=0, has_side_effects=True, vmem_limit_bytes=67043328
            ),
            cost_estimate=pl.CostEstimate(flops=flops, bytes_accessed=0, transcendentals=0),
            name="stage",
        )(x, dy, w_gate, w_up, w_down)
        return by_gate, by_up, jnp.swapaxes(by_down, 1, 2)

    return jax.shard_map(
        step,
        mesh=mesh,
        in_specs=(P("rep", None, None),) * 2 + (P("pp", None, None),) * 3,
        out_specs=(P(("rep", "pp"), None, None),) * 3,
        check_vma=False,
    )
```

```python
import functools

import jax
import jax.numpy as jnp
from jax import lax
from jax.experimental import pallas as pl
from jax.experimental.pallas import tpu as pltpu
from jax.sharding import PartitionSpec as P

f32, bf16 = jnp.float32, jnp.bfloat16
MESH = pl.DeviceIdType.MESH
PARTS = 2
RING_F, RING_B = 4, 2
SENDS = 4
KEPT = 4
STAGES = 8


def ahead_of(me):
    behind = STAGES - 1 - me
    return 2 * behind - behind % 2


def late_of(me):
    return 2 * me


def dot(a, b):
    return jnp.dot(a, b, preferred_element_type=f32)


def dot_t(a, b):
    return lax.dot_general(a, b, (((1,), (1,)), ((), ())), preferred_element_type=f32)


def scale_of(wide):
    return lax.rsqrt(jnp.mean(wide * wide, -1, keepdims=True) + 1e-6)


def kernel(
    x, dy, w_gate, w_up, w_down, by_gate, by_up, by_down, spill, shelf,
    wg, wu, wd, hs, ds, ring, kept, a_t, dy_t, out_f, out_b, sum_g, sum_u, sum_d,
    w_sem, f_recv, b_recv, f_send, b_send, spill_sem, fetch_sem, shelf_sem, unshelf_sem, end_sem,
):
    micro, tokens, d = hs.shape
    ff = wg.shape[1]
    wide_block = 256 if ff % 256 == 0 else 128
    rows_n = tokens // PARTS
    chunks = micro * PARTS
    me = lax.axis_index("pp")
    first, last = me == 0, me == STAGES - 1
    ahead, late = ahead_of(me), late_of(me)
    resident = 2 * ahead + 1 <= RING_F + RING_B
    at_once = late < KEPT
    half = KEPT // 2

    def rows_of(c):
        return pl.ds(c * rows_n, rows_n)

    def weights_in():
        return [
            pltpu.make_async_copy(src.at[0], dst, w_sem.at[i])
            for i, (src, dst) in enumerate(((w_gate, wg), (w_up, wu), (w_down, wd)))
        ]

    def load_x(t, c):
        return pltpu.make_async_copy(x.at[t, rows_of(c)], hs.at[t, rows_of(c)], f_recv.at[t * PARTS + c])

    def load_dy(t, c):
        return pltpu.make_async_copy(dy.at[t, rows_of(c)], ds.at[t, rows_of(c)], b_recv.at[t * PARTS + c])

    def onward(t, c):
        i = t * PARTS + c
        return pltpu.make_async_remote_copy(
            src_ref=out_f.at[i % SENDS],
            dst_ref=hs.at[t, rows_of(c)],
            send_sem=f_send.at[i % SENDS],
            recv_sem=f_recv.at[i],
            device_id={"pp": me + 1},
            device_id_type=MESH,
        )

    def back_again(t, c):
        i = t * PARTS + c
        return pltpu.make_async_remote_copy(
            src_ref=out_b.at[i % SENDS],
            dst_ref=ds.at[t, rows_of(c)],
            send_sem=b_send.at[i % SENDS],
            recv_sem=b_recv.at[i],
            device_id={"pp": me - 1},
            device_id_type=MESH,
        )

    def put_away(i):
        return pltpu.make_async_copy(ring.at[i % RING_F], spill.at[i], spill_sem.at[i % RING_F])

    def fetch(i):
        return pltpu.make_async_copy(spill.at[i], ring.at[RING_F + i % RING_B], fetch_sem.at[i % RING_B])

    def shelve(u):
        return pltpu.make_async_copy(kept.at[u % half], shelf.at[u], shelf_sem.at[u % half])

    def unshelve(v):
        return pltpu.make_async_copy(shelf.at[v], kept.at[half + v % half], unshelf_sem.at[v % half])

    barrier = pltpu.get_barrier_semaphore()

    @pl.when(jnp.logical_not(last))
    def _():
        pl.semaphore_signal(barrier, inc=1, device_id={"pp": me + 1}, device_id_type=MESH)

    @pl.when(jnp.logical_not(first))
    def _():
        pl.semaphore_signal(barrier, inc=1, device_id={"pp": me - 1}, device_id_type=MESH)

    for copy in weights_in():
        copy.start()

    @pl.when(first)
    def _():
        @pl.loop(0, micro)
        def _(t):
            for c in range(PARTS):
                load_x(t, c).start()

    @pl.when(last)
    def _():
        @pl.loop(0, micro)
        def _(t):
            for c in range(PARTS):
                load_dy(t, c).start()

    for total in (sum_g, sum_u, sum_d):
        total[...] = jnp.zeros_like(total)
    for copy in weights_in():
        copy.wait()

    pl.semaphore_wait(barrier, jnp.where(first | last, 1, 2))

    def forward_math(t, c, slot, send):
        rows = rows_of(c)
        wide = hs[t, rows, :].astype(f32)
        a = (wide * scale_of(wide)).astype(bf16)
        products = []
        for n in range(ff // wide_block):
            cols = slice(n * wide_block, (n + 1) * wide_block)
            gate, up = dot(a, wg[:, cols]), dot(a, wu[:, cols])
            ring[slot, 0, :, cols] = gate
            ring[slot, 1, :, cols] = up
            if send:
                products.append((gate * jax.nn.sigmoid(gate) * up).astype(bf16))
        if send:
            y = dot(jnp.concatenate(products, -1), wd[...]).astype(bf16)
            out_f[(t * PARTS + c) % SENDS] = (wide + y.astype(f32)).astype(bf16)

    def forward(t, c):
        i = t * PARTS + c

        @pl.when(first)
        def _():
            load_x(t, c).wait()

        @pl.when(jnp.logical_not(first))
        def _():
            onward(t, c).wait_recv()

        @pl.when(jnp.logical_not(resident) & (i >= RING_F))
        def _():
            put_away(i - RING_F).wait()

        slot = jnp.where(resident, i % (RING_F + RING_B), i % RING_F)

        @pl.when(last)
        def _():
            forward_math(t, c, slot, False)

        @pl.when(jnp.logical_not(last))
        def _():
            @pl.when(i >= SENDS)
            def _():
                back = i - SENDS
                onward(back // PARTS, back % PARTS).wait_send()

            forward_math(t, c, slot, True)
            onward(t, c).start()

        @pl.when(jnp.logical_not(resident))
        def _():
            put_away(i).start()

    def backward_math(t, c, slot, send):
        rows = rows_of(c)
        at = jnp.where(at_once, t % KEPT, t % half)
        by_y = ds[t, rows, :]
        for n in range(ff // wide_block):
            cols = slice(n * wide_block, (n + 1) * wide_block)
            by_product = dot_t(by_y, wd[cols, :]).astype(bf16).astype(f32)
            gate, up = ring[slot, 0, :, cols], ring[slot, 1, :, cols]
            sig = jax.nn.sigmoid(gate)
            silu = gate * sig
            kept[at, 0, rows, cols] = (silu * up).astype(bf16)
            kept[at, 2, rows, cols] = (by_product * silu).astype(bf16)
            kept[at, 1, rows, cols] = (by_product * up * (sig * (1.0 + gate * (1.0 - sig)))).astype(bf16)
        if send:
            by_a = (
                dot_t(kept[at, 1, rows, :], wg[...]).astype(bf16).astype(f32)
                + dot_t(kept[at, 2, rows, :], wu[...]).astype(bf16).astype(f32)
            ).astype(bf16).astype(f32)
            wide = hs[t, rows, :].astype(f32)
            scale = scale_of(wide)
            pull = jnp.sum(by_a * wide, -1, keepdims=True) * (scale * scale * scale) * (-1.0 / d)
            by_h = (by_a * scale + wide * pull).astype(bf16)
            out_b[(t * PARTS + c) % SENDS] = (by_y.astype(f32) + by_h.astype(f32)).astype(bf16)

    def backward(t, c):
        i = t * PARTS + c

        @pl.when(last)
        def _():
            load_dy(t, c).wait()

        @pl.when(jnp.logical_not(last))
        def _():
            back_again(t, c).wait_recv()

        @pl.when(jnp.logical_not(resident))
        def _():
            fetch(i).wait()

            @pl.when(i + 1 < chunks)
            def _():
                fetch(i + 1).start()

        slot = jnp.where(resident, i % (RING_F + RING_B), RING_F + i % RING_B)

        if c == 0:

            @pl.when(jnp.logical_not(at_once) & (t >= half))
            def _():
                shelve(t - half).wait()

        @pl.when(first)
        def _():
            backward_math(t, c, slot, False)

        @pl.when(jnp.logical_not(first))
        def _():
            @pl.when(i >= SENDS)
            def _():
                back = i - SENDS
                back_again(back // PARTS, back % PARTS).wait_send()

            backward_math(t, c, slot, True)
            back_again(t, c).start()

        if c == PARTS - 1:

            @pl.when(jnp.logical_not(at_once))
            def _():
                shelve(t).start()

    def by_weights(t):
        at = jnp.where(at_once, t % KEPT, half + t % half)

        @pl.when(jnp.logical_not(at_once))
        def _():
            unshelve(t).wait()

            @pl.when(t + 1 < micro)
            def _():
                unshelve(t + 1).start()

        wide = hs[t].astype(f32)
        a_t[...] = (wide * scale_of(wide)).astype(bf16).T
        dy_t[...] = ds[t].T
        for i, (total, left) in enumerate(((sum_d, dy_t), (sum_g, a_t), (sum_u, a_t))):
            for n in range(ff // wide_block):
                cols = slice(n * wide_block, (n + 1) * wide_block)
                total[:, cols] += dot(left[...], kept[at, i, :, cols]).astype(bf16).astype(f32)

    @pl.loop(0, micro + max(ahead_of(k) + late_of(k) for k in range(STAGES)))
    def _(t):
        u = t - ahead
        v = u - late

        @pl.when(jnp.logical_not(resident) & (t == micro))
        def _():
            for i in range(chunks - RING_F, chunks):
                put_away(i).wait()

        @pl.when(jnp.logical_not(at_once) & (u == micro))
        def _():
            for i in range(micro - half, micro):
                shelve(i).wait()

        for c in range(PARTS):

            @pl.when(t < micro)
            def _(c=c):
                forward(t, c)

            @pl.when((u >= 0) & (u < micro))
            def _(c=c):
                backward(u, c)

        @pl.when(jnp.logical_not(resident) & (u == -1))
        def _():
            fetch(0).start()

        @pl.when(jnp.logical_not(at_once) & (v == -1))
        def _():
            unshelve(0).start()

        @pl.when((v >= 0) & (v < micro))
        def _():
            by_weights(v)

    copies = []
    for i, (total, out) in enumerate(((sum_g, by_gate), (sum_u, by_up), (sum_d, by_down))):
        kept[0, i] = total[...].astype(bf16)
        copies.append(pltpu.make_async_copy(kept.at[0, i], out.at[0], end_sem.at[i]))
        copies[-1].start()

    @pl.when(jnp.logical_not(last))
    def _():
        for i in range(chunks - SENDS, chunks):
            onward(i // PARTS, i % PARTS).wait_send()

    @pl.when(jnp.logical_not(first))
    def _():
        for i in range(chunks - SENDS, chunks):
            back_again(i // PARTS, i % PARTS).wait_send()

    for copy in copies:
        copy.wait()


def solution(mesh):
    def step(x, dy, w_gate, w_up, w_down):
        micro, tokens, d = x.shape
        ff = w_gate.shape[2]
        rows, chunks = tokens // PARTS, micro * PARTS
        flops = 9 * micro * 2 * tokens * d * ff
        anywhere = pl.BlockSpec(memory_space=pl.ANY)
        by_gate, by_up, by_down, *_ = pl.pallas_call(
            kernel,
            out_shape=[jax.ShapeDtypeStruct((1, d, ff), bf16)] * 3
            + [jax.ShapeDtypeStruct((chunks, 2, rows, ff), f32), jax.ShapeDtypeStruct((micro, 3, tokens, ff), bf16)],
            in_specs=[anywhere] * 5,
            out_specs=[anywhere] * 5,
            scratch_shapes=[
                pltpu.VMEM((d, ff), bf16),
                pltpu.VMEM((d, ff), bf16),
                pltpu.VMEM((ff, d), bf16),
                pltpu.VMEM((micro, tokens, d), bf16),
                pltpu.VMEM((micro, tokens, d), bf16),
                pltpu.VMEM((RING_F + RING_B, 2, rows, ff), f32),
                pltpu.VMEM((KEPT, 3, tokens, ff), bf16),
                pltpu.VMEM((d, tokens), bf16),
                pltpu.VMEM((d, tokens), bf16),
                pltpu.VMEM((SENDS, rows, d), bf16),
                pltpu.VMEM((SENDS, rows, d), bf16),
                *[pltpu.VMEM((d, ff), f32)] * 3,
                pltpu.SemaphoreType.DMA((3,)),
                pltpu.SemaphoreType.DMA((chunks,)),
                pltpu.SemaphoreType.DMA((chunks,)),
                pltpu.SemaphoreType.DMA((SENDS,)),
                pltpu.SemaphoreType.DMA((SENDS,)),
                pltpu.SemaphoreType.DMA((RING_F,)),
                pltpu.SemaphoreType.DMA((RING_B,)),
                pltpu.SemaphoreType.DMA((KEPT // 2,)),
                pltpu.SemaphoreType.DMA((KEPT // 2,)),
                pltpu.SemaphoreType.DMA((3,)),
            ],
            compiler_params=pltpu.CompilerParams(
                collective_id=0, has_side_effects=True, vmem_limit_bytes=67043328
            ),
            cost_estimate=pl.CostEstimate(flops=flops, bytes_accessed=0, transcendentals=0),
            name="stage",
        )(x, dy, w_gate, w_up, w_down)
        return by_gate, by_up, jnp.swapaxes(by_down, 1, 2)

    return jax.shard_map(
        step,
        mesh=mesh,
        in_specs=(P("rep", None, None),) * 2 + (P("pp", None, None),) * 3,
        out_specs=(P(("rep", "pp"), None, None),) * 3,
        check_vma=False,
    )
```

```python
import functools

import jax
import jax.numpy as jnp
from jax import lax
from jax.experimental import pallas as pl
from jax.experimental.pallas import tpu as pltpu
from jax.sharding import PartitionSpec as P

f32, bf16 = jnp.float32, jnp.bfloat16
MESH = pl.DeviceIdType.MESH
PARTS = 2
RING_F, RING_B = 4, 2
SENDS = 4
KEPT = 4
STAGES = 8


def ahead_of(me):
    behind = STAGES - 1 - me
    return 2 * behind - behind % 2


def late_of(me):
    return lax.min((5 * me + 2) // 2, 15)


def dot(a, b):
    return jnp.dot(a, b, preferred_element_type=f32)


def dot_t(a, b):
    return lax.dot_general(a, b, (((1,), (1,)), ((), ())), preferred_element_type=f32)


def scale_of(wide):
    return lax.rsqrt(jnp.mean(wide * wide, -1, keepdims=True) + 1e-6)


def kernel(
    x, dy, w_gate, w_up, w_down, by_gate, by_up, by_down, spill, shelf,
    wg, wu, wd, hs, ds, ring, kept, a_t, dy_t, out_f, out_b, sum_g, sum_u, sum_d,
    w_sem, f_recv, b_recv, f_send, b_send, spill_sem, fetch_sem, shelf_sem, unshelf_sem, end_sem,
):
    micro, tokens, d = hs.shape
    ff = wg.shape[1]
    wide_block = 256 if ff % 256 == 0 else 128
    rows_n = tokens // PARTS
    chunks = micro * PARTS
    me = lax.axis_index("pp")
    first, last = me == 0, me == STAGES - 1
    ahead, late = ahead_of(me), late_of(me)
    resident = 2 * ahead + 1 <= RING_F + RING_B
    at_once = late < KEPT
    half = KEPT // 2

    def rows_of(c):
        return pl.ds(c * rows_n, rows_n)

    def weights_in():
        return [
            pltpu.make_async_copy(src.at[0], dst, w_sem.at[i])
            for i, (src, dst) in enumerate(((w_gate, wg), (w_up, wu), (w_down, wd)))
        ]

    def load_x(t, c):
        return pltpu.make_async_copy(x.at[t, rows_of(c)], hs.at[t, rows_of(c)], f_recv.at[t * PARTS + c])

    def load_dy(t, c):
        return pltpu.make_async_copy(dy.at[t, rows_of(c)], ds.at[t, rows_of(c)], b_recv.at[t * PARTS + c])

    def onward(t, c):
        i = t * PARTS + c
        return pltpu.make_async_remote_copy(
            src_ref=out_f.at[i % SENDS],
            dst_ref=hs.at[t, rows_of(c)],
            send_sem=f_send.at[i % SENDS],
            recv_sem=f_recv.at[i],
            device_id={"pp": me + 1},
            device_id_type=MESH,
        )

    def back_again(t, c):
        i = t * PARTS + c
        return pltpu.make_async_remote_copy(
            src_ref=out_b.at[i % SENDS],
            dst_ref=ds.at[t, rows_of(c)],
            send_sem=b_send.at[i % SENDS],
            recv_sem=b_recv.at[i],
            device_id={"pp": me - 1},
            device_id_type=MESH,
        )

    def put_away(i):
        return pltpu.make_async_copy(ring.at[i % RING_F], spill.at[i], spill_sem.at[i % RING_F])

    def fetch(i):
        return pltpu.make_async_copy(spill.at[i], ring.at[RING_F + i % RING_B], fetch_sem.at[i % RING_B])

    def shelve(u):
        return pltpu.make_async_copy(kept.at[u % half], shelf.at[u], shelf_sem.at[u % half])

    def unshelve(v):
        return pltpu.make_async_copy(shelf.at[v], kept.at[half + v % half], unshelf_sem.at[v % half])

    barrier = pltpu.get_barrier_semaphore()

    @pl.when(jnp.logical_not(last))
    def _():
        pl.semaphore_signal(barrier, inc=1, device_id={"pp": me + 1}, device_id_type=MESH)

    @pl.when(jnp.logical_not(first))
    def _():
        pl.semaphore_signal(barrier, inc=1, device_id={"pp": me - 1}, device_id_type=MESH)

    for copy in weights_in():
        copy.start()

    @pl.when(first)
    def _():
        @pl.loop(0, micro)
        def _(t):
            for c in range(PARTS):
                load_x(t, c).start()

    @pl.when(last)
    def _():
        @pl.loop(0, micro)
        def _(t):
            for c in range(PARTS):
                load_dy(t, c).start()

    def clear():
        for total in (sum_g, sum_u, sum_d):
            total[...] = jnp.zeros_like(total)

    @pl.when(jnp.logical_not(first))
    def _():
        clear()

    for copy in weights_in():
        copy.wait()

    pl.semaphore_wait(barrier, jnp.where(first | last, 1, 2))

    def forward_math(t, c, slot, send):
        rows = rows_of(c)
        wide = hs[t, rows, :].astype(f32)
        a = (wide * scale_of(wide)).astype(bf16)
        products = []
        for n in range(ff // wide_block):
            cols = slice(n * wide_block, (n + 1) * wide_block)
            gate, up = dot(a, wg[:, cols]), dot(a, wu[:, cols])
            ring[slot, 0, :, cols] = gate
            ring[slot, 1, :, cols] = up
            if send:
                products.append((gate * jax.nn.sigmoid(gate) * up).astype(bf16))
        if send:
            y = dot(jnp.concatenate(products, -1), wd[...]).astype(bf16)
            out_f[(t * PARTS + c) % SENDS] = (wide + y.astype(f32)).astype(bf16)

    def forward(t, c):
        i = t * PARTS + c

        @pl.when(first)
        def _():
            load_x(t, c).wait()

        @pl.when(jnp.logical_not(first))
        def _():
            onward(t, c).wait_recv()

        @pl.when(jnp.logical_not(resident) & (i >= RING_F))
        def _():
            put_away(i - RING_F).wait()

        slot = jnp.where(resident, i % (RING_F + RING_B), i % RING_F)

        @pl.when(last)
        def _():
            forward_math(t, c, slot, False)

        @pl.when(jnp.logical_not(last))
        def _():
            @pl.when(i >= SENDS)
            def _():
                back = i - SENDS
                onward(back // PARTS, back % PARTS).wait_send()

            forward_math(t, c, slot, True)
            onward(t, c).start()

        @pl.when(jnp.logical_not(resident))
        def _():
            put_away(i).start()

    def backward_math(t, c, slot, send):
        rows = rows_of(c)
        at = jnp.where(at_once, t % KEPT, t % half)
        by_y = ds[t, rows, :]
        for n in range(ff // wide_block):
            cols = slice(n * wide_block, (n + 1) * wide_block)
            by_product = dot_t(by_y, wd[cols, :]).astype(bf16).astype(f32)
            gate, up = ring[slot, 0, :, cols], ring[slot, 1, :, cols]
            sig = jax.nn.sigmoid(gate)
            silu = gate * sig
            kept[at, 0, rows, cols] = (silu * up).astype(bf16)
            kept[at, 2, rows, cols] = (by_product * silu).astype(bf16)
            kept[at, 1, rows, cols] = (by_product * up * (sig * (1.0 + gate * (1.0 - sig)))).astype(bf16)
        if send:
            by_a = (
                dot_t(kept[at, 1, rows, :], wg[...]).astype(bf16).astype(f32)
                + dot_t(kept[at, 2, rows, :], wu[...]).astype(bf16).astype(f32)
            ).astype(bf16).astype(f32)
            wide = hs[t, rows, :].astype(f32)
            scale = scale_of(wide)
            pull = jnp.sum(by_a * wide, -1, keepdims=True) * (scale * scale * scale) * (-1.0 / d)
            by_h = (by_a * scale + wide * pull).astype(bf16)
            out_b[(t * PARTS + c) % SENDS] = (by_y.astype(f32) + by_h.astype(f32)).astype(bf16)

    def backward(t, c):
        i = t * PARTS + c

        @pl.when(last)
        def _():
            load_dy(t, c).wait()

        @pl.when(jnp.logical_not(last))
        def _():
            back_again(t, c).wait_recv()

        @pl.when(jnp.logical_not(resident))
        def _():
            fetch(i).wait()

            @pl.when(i + 1 < chunks)
            def _():
                fetch(i + 1).start()

        slot = jnp.where(resident, i % (RING_F + RING_B), RING_F + i % RING_B)

        if c == 0:

            @pl.when(jnp.logical_not(at_once) & (t >= half))
            def _():
                shelve(t - half).wait()

        @pl.when(first)
        def _():
            backward_math(t, c, slot, False)

        @pl.when(jnp.logical_not(first))
        def _():
            @pl.when(i >= SENDS)
            def _():
                back = i - SENDS
                back_again(back // PARTS, back % PARTS).wait_send()

            backward_math(t, c, slot, True)
            back_again(t, c).start()

        if c == PARTS - 1:

            @pl.when(jnp.logical_not(at_once))
            def _():
                shelve(t).start()

    def by_weights(t):
        at = jnp.where(at_once, t % KEPT, half + t % half)

        @pl.when(jnp.logical_not(at_once))
        def _():
            unshelve(t).wait()

            @pl.when(t + 1 < micro)
            def _():
                unshelve(t + 1).start()

        wide = hs[t].astype(f32)
        a_t[...] = (wide * scale_of(wide)).astype(bf16).T
        dy_t[...] = ds[t].T
        for i, (total, left) in enumerate(((sum_d, dy_t), (sum_g, a_t), (sum_u, a_t))):
            for n in range(ff // wide_block):
                cols = slice(n * wide_block, (n + 1) * wide_block)
                total[:, cols] += dot(left[...], kept[at, i, :, cols]).astype(bf16).astype(f32)

    @pl.loop(0, micro + max(ahead_of(k) + min((5 * k + 2) // 2, 15) for k in range(STAGES)))
    def _(t):
        u = t - ahead
        v = u - late

        @pl.when(jnp.logical_not(resident) & (t == micro))
        def _():
            for i in range(chunks - RING_F, chunks):
                put_away(i).wait()

        @pl.when(first & (t == 4))
        def _():
            clear()

        @pl.when(jnp.logical_not(at_once) & (u == micro))
        def _():
            for i in range(micro - half, micro):
                shelve(i).wait()

        for c in range(PARTS):

            @pl.when(t < micro)
            def _(c=c):
                forward(t, c)

            @pl.when((u >= 0) & (u < micro))
            def _(c=c):
                backward(u, c)

        @pl.when(jnp.logical_not(resident) & (u == -1))
        def _():
            fetch(0).start()

        @pl.when(jnp.logical_not(at_once) & (v == -1))
        def _():
            unshelve(0).start()

        @pl.when((v >= 0) & (v < micro))
        def _():
            by_weights(v)

    copies = []
    for i, (total, out) in enumerate(((sum_g, by_gate), (sum_u, by_up), (sum_d, by_down))):
        kept[0, i] = total[...].astype(bf16)
        copies.append(pltpu.make_async_copy(kept.at[0, i], out.at[0], end_sem.at[i]))
        copies[-1].start()

    @pl.when(jnp.logical_not(last))
    def _():
        for i in range(chunks - SENDS, chunks):
            onward(i // PARTS, i % PARTS).wait_send()

    @pl.when(jnp.logical_not(first))
    def _():
        for i in range(chunks - SENDS, chunks):
            back_again(i // PARTS, i % PARTS).wait_send()

    for copy in copies:
        copy.wait()


def hand_out(g, u, d, by_gate, by_up, by_down):
    by_gate[...] = g[...]
    by_up[...] = u[...]
    by_down[0] = d[0].T


def solution(mesh):
    def step(x, dy, w_gate, w_up, w_down):
        micro, tokens, d = x.shape
        ff = w_gate.shape[2]
        rows, chunks = tokens // PARTS, micro * PARTS
        flops = 9 * micro * 2 * tokens * d * ff
        anywhere = pl.BlockSpec(memory_space=pl.ANY)
        by_gate, by_up, by_down, *_ = pl.pallas_call(
            kernel,
            out_shape=[jax.ShapeDtypeStruct((1, d, ff), bf16)] * 3
            + [jax.ShapeDtypeStruct((chunks, 2, rows, ff), f32), jax.ShapeDtypeStruct((micro, 3, tokens, ff), bf16)],
            in_specs=[anywhere] * 5,
            out_specs=[anywhere] * 5,
            scratch_shapes=[
                pltpu.VMEM((d, ff), bf16),
                pltpu.VMEM((d, ff), bf16),
                pltpu.VMEM((ff, d), bf16),
                pltpu.VMEM((micro, tokens, d), bf16),
                pltpu.VMEM((micro, tokens, d), bf16),
                pltpu.VMEM((RING_F + RING_B, 2, rows, ff), f32),
                pltpu.VMEM((KEPT, 3, tokens, ff), bf16),
                pltpu.VMEM((d, tokens), bf16),
                pltpu.VMEM((d, tokens), bf16),
                pltpu.VMEM((SENDS, rows, d), bf16),
                pltpu.VMEM((SENDS, rows, d), bf16),
                *[pltpu.VMEM((d, ff), f32)] * 3,
                pltpu.SemaphoreType.DMA((3,)),
                pltpu.SemaphoreType.DMA((chunks,)),
                pltpu.SemaphoreType.DMA((chunks,)),
                pltpu.SemaphoreType.DMA((SENDS,)),
                pltpu.SemaphoreType.DMA((SENDS,)),
                pltpu.SemaphoreType.DMA((RING_F,)),
                pltpu.SemaphoreType.DMA((RING_B,)),
                pltpu.SemaphoreType.DMA((KEPT // 2,)),
                pltpu.SemaphoreType.DMA((KEPT // 2,)),
                pltpu.SemaphoreType.DMA((3,)),
            ],
            compiler_params=pltpu.CompilerParams(
                collective_id=0, has_side_effects=True, vmem_limit_bytes=67043328
            ),
            cost_estimate=pl.CostEstimate(flops=flops, bytes_accessed=0, transcendentals=0),
            name="stage",
        )(x, dy, w_gate, w_up, w_down)
        across = pl.BlockSpec((1, d, 256), lambda i: (0, 0, i))
        return pl.pallas_call(
            hand_out,
            grid=(ff // 256,),
            out_shape=[jax.ShapeDtypeStruct((1, d, ff), bf16)] * 2 + [jax.ShapeDtypeStruct((1, ff, d), bf16)],
            in_specs=[across] * 3,
            out_specs=[across] * 2 + [pl.BlockSpec((1, 256, d), lambda i: (0, i, 0))],
            name="hand_out",
        )(by_gate, by_up, by_down)

    return jax.shard_map(
        step,
        mesh=mesh,
        in_specs=(P("rep", None, None),) * 2 + (P("pp", None, None),) * 3,
        out_specs=(P(("rep", "pp"), None, None),) * 3,
        check_vma=False,
    )
```

```python
import functools

import jax
import jax.numpy as jnp
from jax import lax
from jax.experimental import pallas as pl
from jax.experimental.pallas import tpu as pltpu
from jax.sharding import PartitionSpec as P

f32, bf16 = jnp.float32, jnp.bfloat16
MESH = pl.DeviceIdType.MESH
PARTS = 2
RING_F, RING_B = 4, 2
SENDS = 4
KEPT = 4
STAGES = 8


def ahead_of(me):
    behind = STAGES - 1 - me
    return 2 * behind - behind % 2


def late_of(me):
    return lax.min((5 * me + 2) // 2, 15)


def dot(a, b):
    return jnp.dot(a, b, preferred_element_type=f32)


def dot_t(a, b):
    return lax.dot_general(a, b, (((1,), (1,)), ((), ())), preferred_element_type=f32)


def scale_of(wide):
    return lax.rsqrt(jnp.mean(wide * wide, -1, keepdims=True) + 1e-6)


def kernel(
    x, dy, w_gate, w_up, w_down, by_gate, by_up, by_down, spill, shelf,
    wg, wu, wd, hs, ds, ring, kept, a_t, dy_t, out_f, out_b, sum_g, sum_u, sum_d,
    w_sem, f_recv, b_recv, f_send, b_send, spill_sem, fetch_sem, shelf_sem, unshelf_sem, end_sem,
):
    micro, tokens, d = hs.shape
    ff = wg.shape[1]
    wide_block = 256 if ff % 256 == 0 else 128
    rows_n = tokens // PARTS
    chunks = micro * PARTS
    me = lax.axis_index("pp")
    first, last = me == 0, me == STAGES - 1
    ahead, late = ahead_of(me), late_of(me)
    resident = 2 * ahead + 1 <= RING_F + RING_B
    at_once = late < KEPT
    half = KEPT // 2

    def rows_of(c):
        return pl.ds(c * rows_n, rows_n)

    def weights_in():
        return [
            pltpu.make_async_copy(src.at[0], dst, w_sem.at[i])
            for i, (src, dst) in enumerate(((w_gate, wg), (w_up, wu), (w_down, wd)))
        ]

    def load_x(t, c):
        return pltpu.make_async_copy(x.at[t, rows_of(c)], hs.at[t, rows_of(c)], f_recv.at[t * PARTS + c])

    def load_dy(t, c):
        return pltpu.make_async_copy(dy.at[t, rows_of(c)], ds.at[t, rows_of(c)], b_recv.at[t * PARTS + c])

    def onward(t, c):
        i = t * PARTS + c
        return pltpu.make_async_remote_copy(
            src_ref=out_f.at[i % SENDS],
            dst_ref=hs.at[t, rows_of(c)],
            send_sem=f_send.at[i % SENDS],
            recv_sem=f_recv.at[i],
            device_id={"pp": me + 1},
            device_id_type=MESH,
        )

    def back_again(t, c):
        i = t * PARTS + c
        return pltpu.make_async_remote_copy(
            src_ref=out_b.at[i % SENDS],
            dst_ref=ds.at[t, rows_of(c)],
            send_sem=b_send.at[i % SENDS],
            recv_sem=b_recv.at[i],
            device_id={"pp": me - 1},
            device_id_type=MESH,
        )

    def put_away(i):
        return pltpu.make_async_copy(ring.at[i % RING_F], spill.at[i], spill_sem.at[i % RING_F])

    def fetch(i):
        return pltpu.make_async_copy(spill.at[i], ring.at[RING_F + i % RING_B], fetch_sem.at[i % RING_B])

    def shelve(u):
        return pltpu.make_async_copy(kept.at[u % half], shelf.at[u], shelf_sem.at[u % half])

    def unshelve(v):
        return pltpu.make_async_copy(shelf.at[v], kept.at[half + v % half], unshelf_sem.at[v % half])

    barrier = pltpu.get_barrier_semaphore()

    @pl.when(jnp.logical_not(last))
    def _():
        pl.semaphore_signal(barrier, inc=1, device_id={"pp": me + 1}, device_id_type=MESH)

    @pl.when(jnp.logical_not(first))
    def _():
        pl.semaphore_signal(barrier, inc=1, device_id={"pp": me - 1}, device_id_type=MESH)

    for copy in weights_in():
        copy.start()

    @pl.when(first)
    def _():
        @pl.loop(0, micro)
        def _(t):
            for c in range(PARTS):
                load_x(t, c).start()

    @pl.when(last)
    def _():
        @pl.loop(0, micro)
        def _(t):
            for c in range(PARTS):
                load_dy(t, c).start()

    def clear():
        for total in (sum_g, sum_u, sum_d):
            total[...] = jnp.zeros_like(total)

    @pl.when(jnp.logical_not(first))
    def _():
        clear()

    for copy in weights_in():
        copy.wait()

    pl.semaphore_wait(barrier, jnp.where(first | last, 1, 2))

    def forward_math(t, c, slot, send):
        rows = rows_of(c)
        wide = hs[t, rows, :].astype(f32)
        a = (wide * scale_of(wide)).astype(bf16)
        products = []
        for n in range(ff // wide_block):
            cols = slice(n * wide_block, (n + 1) * wide_block)
            gate, up = dot(a, wg[:, cols]), dot(a, wu[:, cols])
            ring[slot, 0, :, cols] = gate
            ring[slot, 1, :, cols] = up
            if send:
                products.append((gate * jax.nn.sigmoid(gate) * up).astype(bf16))
        if send:
            y = dot(jnp.concatenate(products, -1), wd[...]).astype(bf16)
            out_f[(t * PARTS + c) % SENDS] = (wide + y.astype(f32)).astype(bf16)

    def forward(t, c):
        i = t * PARTS + c

        @pl.when(first)
        def _():
            load_x(t, c).wait()

        @pl.when(jnp.logical_not(first))
        def _():
            onward(t, c).wait_recv()

        @pl.when(jnp.logical_not(resident) & (i >= RING_F))
        def _():
            put_away(i - RING_F).wait()

        slot = jnp.where(resident, i % (RING_F + RING_B), i % RING_F)

        @pl.when(last)
        def _():
            forward_math(t, c, slot, False)

        @pl.when(jnp.logical_not(last))
        def _():
            @pl.when(i >= SENDS)
            def _():
                back = i - SENDS
                onward(back // PARTS, back % PARTS).wait_send()

            forward_math(t, c, slot, True)
            onward(t, c).start()

        @pl.when(jnp.logical_not(resident))
        def _():
            put_away(i).start()

    def backward_math(t, c, slot, send):
        rows = rows_of(c)
        at = jnp.where(at_once, t % KEPT, t % half)
        by_y = ds[t, rows, :]
        for n in range(ff // wide_block):
            cols = slice(n * wide_block, (n + 1) * wide_block)
            by_product = dot_t(by_y, wd[cols, :]).astype(bf16).astype(f32)
            gate, up = ring[slot, 0, :, cols], ring[slot, 1, :, cols]
            sig = jax.nn.sigmoid(gate)
            silu = gate * sig
            kept[at, 0, rows, cols] = (silu * up).astype(bf16)
            kept[at, 2, rows, cols] = (by_product * silu).astype(bf16)
            kept[at, 1, rows, cols] = (by_product * up * (sig * (1.0 + gate * (1.0 - sig)))).astype(bf16)
        if send:
            by_a = (
                dot_t(kept[at, 1, rows, :], wg[...]).astype(bf16).astype(f32)
                + dot_t(kept[at, 2, rows, :], wu[...]).astype(bf16).astype(f32)
            ).astype(bf16).astype(f32)
            wide = hs[t, rows, :].astype(f32)
            scale = scale_of(wide)
            pull = jnp.sum(by_a * wide, -1, keepdims=True) * (scale * scale * scale) * (-1.0 / d)
            by_h = (by_a * scale + wide * pull).astype(bf16)
            out_b[(t * PARTS + c) % SENDS] = (by_y.astype(f32) + by_h.astype(f32)).astype(bf16)

    def backward(t, c):
        i = t * PARTS + c

        @pl.when(last)
        def _():
            load_dy(t, c).wait()

        @pl.when(jnp.logical_not(last))
        def _():
            back_again(t, c).wait_recv()

        @pl.when(jnp.logical_not(resident))
        def _():
            fetch(i).wait()

            @pl.when(i + 1 < chunks)
            def _():
                fetch(i + 1).start()

        slot = jnp.where(resident, i % (RING_F + RING_B), RING_F + i % RING_B)

        if c == 0:

            @pl.when(jnp.logical_not(at_once) & (t >= half))
            def _():
                shelve(t - half).wait()

        @pl.when(first)
        def _():
            backward_math(t, c, slot, False)

        @pl.when(jnp.logical_not(first))
        def _():
            @pl.when(i >= SENDS)
            def _():
                back = i - SENDS
                back_again(back // PARTS, back % PARTS).wait_send()

            backward_math(t, c, slot, True)
            back_again(t, c).start()

        if c == PARTS - 1:

            @pl.when(jnp.logical_not(at_once))
            def _():
                shelve(t).start()

    def by_weights(t):
        at = jnp.where(at_once, t % KEPT, half + t % half)

        @pl.when(jnp.logical_not(at_once))
        def _():
            unshelve(t).wait()

            @pl.when(t + 1 < micro)
            def _():
                unshelve(t + 1).start()

        wide = hs[t].astype(f32)
        a_t[...] = (wide * scale_of(wide)).astype(bf16).T
        dy_t[...] = ds[t].T
        for i, (total, left) in enumerate(((sum_d, dy_t), (sum_g, a_t), (sum_u, a_t))):
            for n in range(ff // wide_block):
                cols = slice(n * wide_block, (n + 1) * wide_block)
                total[:, cols] += dot(left[...], kept[at, i, :, cols]).astype(bf16).astype(f32)

    @pl.loop(0, micro + max(ahead_of(k) + min((5 * k + 2) // 2, 15) for k in range(STAGES)))
    def _(t):
        u = t - ahead
        v = u - late

        @pl.when(jnp.logical_not(resident) & (t == micro))
        def _():
            for i in range(chunks - RING_F, chunks):
                put_away(i).wait()

        @pl.when(first & (t == 4))
        def _():
            clear()

        @pl.when(jnp.logical_not(at_once) & (u == micro))
        def _():
            for i in range(micro - half, micro):
                shelve(i).wait()

        for c in range(PARTS):

            @pl.when(t < micro)
            def _(c=c):
                forward(t, c)

            @pl.when((u >= 0) & (u < micro))
            def _(c=c):
                backward(u, c)

        @pl.when(jnp.logical_not(resident) & (u == -1))
        def _():
            fetch(0).start()

        @pl.when(jnp.logical_not(at_once) & (v == -1))
        def _():
            unshelve(0).start()

        @pl.when((v >= 0) & (v < micro))
        def _():
            by_weights(v)

    copies = []
    for i, (total, out) in enumerate(((sum_g, by_gate), (sum_u, by_up), (sum_d, by_down))):
        kept[0, i] = total[...].astype(bf16)
        copies.append(pltpu.make_async_copy(kept.at[0, i], out.at[0], end_sem.at[i]))
        copies[-1].start()

    @pl.when(jnp.logical_not(last))
    def _():
        for i in range(chunks - SENDS, chunks):
            onward(i // PARTS, i % PARTS).wait_send()

    @pl.when(jnp.logical_not(first))
    def _():
        for i in range(chunks - SENDS, chunks):
            back_again(i // PARTS, i % PARTS).wait_send()

    for copy in copies:
        copy.wait()


def solution(mesh):
    def step(x, dy, w_gate, w_up, w_down):
        micro, tokens, d = x.shape
        ff = w_gate.shape[2]
        rows, chunks = tokens // PARTS, micro * PARTS
        flops = 9 * micro * 2 * tokens * d * ff
        anywhere = pl.BlockSpec(memory_space=pl.ANY)
        by_gate, by_up, by_down, *_ = pl.pallas_call(
            kernel,
            out_shape=[jax.ShapeDtypeStruct((1, d, ff), bf16)] * 3
            + [jax.ShapeDtypeStruct((chunks, 2, rows, ff), f32), jax.ShapeDtypeStruct((micro, 3, tokens, ff), bf16)],
            in_specs=[anywhere] * 5,
            out_specs=[anywhere] * 5,
            scratch_shapes=[
                pltpu.VMEM((d, ff), bf16),
                pltpu.VMEM((d, ff), bf16),
                pltpu.VMEM((ff, d), bf16),
                pltpu.VMEM((micro, tokens, d), bf16),
                pltpu.VMEM((micro, tokens, d), bf16),
                pltpu.VMEM((RING_F + RING_B, 2, rows, ff), f32),
                pltpu.VMEM((KEPT, 3, tokens, ff), bf16),
                pltpu.VMEM((d, tokens), bf16),
                pltpu.VMEM((d, tokens), bf16),
                pltpu.VMEM((SENDS, rows, d), bf16),
                pltpu.VMEM((SENDS, rows, d), bf16),
                *[pltpu.VMEM((d, ff), f32)] * 3,
                pltpu.SemaphoreType.DMA((3,)),
                pltpu.SemaphoreType.DMA((chunks,)),
                pltpu.SemaphoreType.DMA((chunks,)),
                pltpu.SemaphoreType.DMA((SENDS,)),
                pltpu.SemaphoreType.DMA((SENDS,)),
                pltpu.SemaphoreType.DMA((RING_F,)),
                pltpu.SemaphoreType.DMA((RING_B,)),
                pltpu.SemaphoreType.DMA((KEPT // 2,)),
                pltpu.SemaphoreType.DMA((KEPT // 2,)),
                pltpu.SemaphoreType.DMA((3,)),
            ],
            compiler_params=pltpu.CompilerParams(
                collective_id=0, has_side_effects=True, vmem_limit_bytes=67043328
            ),
            cost_estimate=pl.CostEstimate(flops=flops, bytes_accessed=0, transcendentals=0),
            name="stage",
        )(x, dy, w_gate, w_up, w_down)
        return by_gate, by_up, jnp.swapaxes(by_down, 1, 2)

    return jax.shard_map(
        step,
        mesh=mesh,
        in_specs=(P("rep", None, None),) * 2 + (P("pp", None, None),) * 3,
        out_specs=(P(("rep", "pp"), None, None),) * 3,
        check_vma=False,
    )
```
